32 devices in a mesh: gx: 4 (over x, core), gy: 8 (over z, y).
Axes of the slice: x: 2, y: 2, z: 4, core: 2. Of those that a mesh axis runs over, the one named last changes fastest.
Arguments:
- state: float32 [256, 2, 128, 128], P(('gx', 'gy')), may hold values from -6 to 6
- hamiltonian: float32 [2, 128, 128], replicated, may hold values from -0.5 to 0.5
- couplings: float32 [16, 128, 128], replicated, may hold values from -0.125 to 0.125
- bath_coef: float32 [2, 16], replicated, may hold values from 0.2 to 1
- bath_rate: float32 [16], replicated, may hold values from 0.02 to 0.2
- occupation: int32 [256, 16], P(('gx', 'gy')), may hold values from 0 to 5
- send_list: int32 [32, 32, 1], P(('gx', 'gy')), may hold values from -1 to 7
- up_index: int32 [256, 16], P(('gx', 'gy')), may hold values from -1 to 39
- down_index: int32 [256, 16], P(('gx', 'gy')), may hold values from -1 to 39
- step: float32 [1], replicated, may hold values from 0.5 to 1.5
Outputs:
- derivative: float32 [256, 2, 128, 128], P(('gx', 'gy'))
- advanced: float32 [256, 2, 128, 128], P(('gx', 'gy'))
The draws below stay inside these ranges and needn't reach their ends.
All inputs are finite; a program needn't handle non-finite values.
Results may differ from the reference program's by a relative error of at most 0.0003.
Values sent between devices are 32-bit elements; how exact they have to be, the bound alone decides.
A program may use at most 256 MiB of HBM per device.

```python
import math
import jax
import jax.numpy as jnp
from jax import lax

NS = 128
K = 16
M_DEV = 8
S = 1
TOTAL = 256


def draw_occupation(key, part):
    devices = TOTAL // M_DEV
    owner = jnp.arange(TOTAL, dtype=jnp.int32) // M_DEV
    highest = jnp.minimum(1 + 5 * owner // max(devices - 1, 1), 5)
    tops = jnp.broadcast_to((highest + 1)[:, None], (TOTAL, K))
    values = jax.random.randint(jax.random.fold_in(key, 11), (TOTAL, K), 0, 6)
    values = jnp.minimum(values, tops - 1)
    return values.at[TOTAL - 1, 0].set(5).astype(jnp.int32)


def draw_send_list(key, part):
    devices = TOTAL // M_DEV
    values = jax.random.randint(jax.random.fold_in(key, 21), (devices, devices, S), 0, M_DEV)
    keep = jax.random.randint(jax.random.fold_in(key, 22), (devices, devices, S), 0, 10) < 7
    values = jnp.where(keep, values, -1)
    values = values.at[0, 0, 0].set(M_DEV - 1).at[0, 1, 0].set(-1)
    return values.astype(jnp.int32)


def neighbour_draw(key, salt):
    devices = TOTAL // M_DEV
    kind = jax.random.randint(jax.random.fold_in(key, salt), (TOTAL, K), 0, 10)
    local = jax.random.randint(jax.random.fold_in(key, salt + 1), (TOTAL, K), 0, M_DEV)
    remote = M_DEV + jax.random.randint(jax.random.fold_in(key, salt + 2), (TOTAL, K), 0, devices * S)
    values = jnp.where(kind < 1, -1, jnp.where(kind < 5, local, remote))
    values = values.at[0, 0].set(M_DEV + devices * S - 1).at[0, 1].set(-1)
    return values.astype(jnp.int32)


def draw_up_index(key, part):
    return neighbour_draw(key, 31)


def draw_down_index(key, part):
    return neighbour_draw(key, 41)


def steps_of(stream_key, extent, pieces, smallest, high):
    gain = 1.0
    for dim, shards_of in pieces:
        steps = jax.random.uniform(jax.random.fold_in(jax.random.fold_in(stream_key, 6), dim), (shards_of,), jnp.float32, smallest / len(pieces), high / len(pieces))
        gain = gain * jnp.repeat(jnp.exp(steps), extent[dim] // shards_of).reshape((-1,) + (1,) * (len(extent) - 1 - dim))
    return gain


def gaussian(stream_key, extent, spread, bound, pieces=(), kind=jnp.bfloat16):
    gain = steps_of(stream_key, extent, pieces, -0.22, 0.18) if pieces else 1.0
    result = jax.random.normal(stream_key, extent, jnp.float32) * spread * gain
    return jnp.minimum(jnp.maximum(result, -bound), bound).astype(kind)


def setup_inputs(seed: int = 0) -> dict:
    splits = jax.random.split(jax.random.key(seed), 11)
    return {
        "state": gaussian(splits[0], (TOTAL, 2, NS, NS), 1.0, 6.0, ((0, 32),), jnp.float32),
        "hamiltonian": gaussian(splits[1], (2, NS, NS), NS ** -0.5, 0.5, (), jnp.float32),
        "couplings": gaussian(splits[2], (K, NS, NS), (NS * K) ** -0.5, 0.125, (), jnp.float32),
        "bath_coef": jnp.clip(jax.random.uniform(splits[3], (2, K), jnp.float32, 0.2, 1.0), 0.2, 1.0),
        "bath_rate": jnp.clip(jnp.exp(jax.random.uniform(splits[4], (K,), jnp.float32, math.log(0.02), math.log(0.2))), 0.02, 0.2),
        "occupation": draw_occupation(jax.random.fold_in(splits[10], 71), 0),
        "send_list": draw_send_list(jax.random.fold_in(splits[10], 71), 0),
        "up_index": draw_up_index(jax.random.fold_in(splits[10], 71), 0),
        "down_index": draw_down_index(jax.random.fold_in(splits[10], 71), 0),
        "step": jnp.clip(jax.random.uniform(splits[9], (1,), jnp.float32, 0.5, 1.5), 0.5, 1.5),
    }


def left_product(matrix, rows):
    return jnp.einsum('ij,mcjl->mcil', matrix, rows, precision=lax.Precision.HIGHEST)

def right_product(rows, matrix):
    return jnp.einsum('mcij,jl->mcil', rows, matrix, precision=lax.Precision.HIGHEST)

def derive(local, buffer, occupation, up_index, down_index, hamiltonian, couplings, bath_coef, bath_rate):
    counts = occupation.astype(local.dtype)
    modes = couplings.shape[0]
    rows = local.shape[0]
    joined = jnp.concatenate([up_index, down_index], axis=1).T.reshape(-1)
    picked = jnp.take(buffer, jnp.clip(joined, 0, buffer.shape[0] - 1).astype(jnp.int32), axis=0)
    picked = picked * (joined >= 0).astype(buffer.dtype)[:, None, None, None]
    picked = picked.reshape((2 * modes, rows) + local.shape[1:])
    stacked = jnp.concatenate([couplings, couplings], axis=0)
    lefts = jnp.einsum('kij,kmcjl->kmcil', stacked, picked, precision=lax.Precision.HIGHEST)
    rights = jnp.einsum('kmcij,kjl->kmcil', picked, stacked, precision=lax.Precision.HIGHEST)
    comm = lax.optimization_barrier(jnp.sum(lefts[:modes] - rights[:modes], axis=0))
    left_low, right_low = (lefts[modes:], rights[modes:])
    coef_real = bath_coef[0][:, None, None, None]
    coef_imag = bath_coef[1][:, None, None, None]
    part_x = coef_real * (left_low[:, :, 0] - right_low[:, :, 0]) - coef_imag * (left_low[:, :, 1] + right_low[:, :, 1])
    part_y = coef_real * (left_low[:, :, 1] - right_low[:, :, 1]) + coef_imag * (left_low[:, :, 0] + right_low[:, :, 0])
    weight = counts.T[:, :, None, None]
    sum_x = lax.optimization_barrier(jnp.sum(weight * part_x, axis=0))
    sum_y = lax.optimization_barrier(jnp.sum(weight * part_y, axis=0))
    total = jnp.stack([comm[:, 1] + sum_y, -comm[:, 0] - sum_x], axis=1)
    ham_real, ham_imag = (hamiltonian[0], hamiltonian[1])
    real_part, imag_part = (local[:, 0:1], local[:, 1:2])
    left_real = left_product(ham_real, real_part) - left_product(ham_imag, imag_part)
    left_imag = left_product(ham_real, imag_part) + left_product(ham_imag, real_part)
    right_real = right_product(real_part, ham_real) - right_product(imag_part, ham_imag)
    right_imag = right_product(real_part, ham_imag) + right_product(imag_part, ham_real)
    comm_real = left_real - right_real
    comm_imag = left_imag - right_imag
    total = total + jnp.concatenate([comm_imag, -comm_real], axis=1)
    damping = lax.optimization_barrier(jnp.sum(counts * bath_rate[None, :], axis=1))
    return total - damping[:, None, None, None] * local

def reference(state, hamiltonian, couplings, bath_coef, bath_rate, occupation, send_list, up_index, down_index, step):
    devices = TOTAL // M_DEV

    def one_device(dev):
        local = lax.dynamic_slice_in_dim(state, dev * M_DEV, M_DEV, 0)
        chosen = lax.dynamic_index_in_dim(send_list, dev, 1, keepdims=False)
        owners = jnp.arange(devices, dtype=jnp.int32)[:, None]
        flat = owners * M_DEV + jnp.clip(chosen, 0, M_DEV - 1).astype(jnp.int32)
        arrived = jnp.take(state, flat.reshape(-1), axis=0)
        arrived = arrived * (chosen.reshape(-1) >= 0).astype(state.dtype)[:, None, None, None]
        buffer = jnp.concatenate([local, arrived], axis=0)
        occ = lax.dynamic_slice_in_dim(occupation, dev * M_DEV, M_DEV, 0)
        ups = lax.dynamic_slice_in_dim(up_index, dev * M_DEV, M_DEV, 0)
        downs = lax.dynamic_slice_in_dim(down_index, dev * M_DEV, M_DEV, 0)
        return derive(local, buffer, occ, ups, downs, hamiltonian, couplings, bath_coef, bath_rate)
    parts = lax.map(one_device, jnp.arange(devices, dtype=jnp.int32))
    derivative = parts.reshape(state.shape)
    count = TOTAL * 2 * NS * NS
    rms = jnp.sqrt(jnp.sum(derivative * derivative) / count + 1e-06)
    advanced = state + step[0] / rms * derivative
    return (derivative, advanced)
```

```python
import functools

import jax
import jax.numpy as jnp
from jax import lax
from jax.experimental import pallas as pl
from jax.experimental.pallas import tpu as pltpu
from jax.sharding import PartitionSpec as P

AXES = ("gx", "gy")
MESH = pl.DeviceIdType.MESH


def split(value):
    high = value.astype(jnp.bfloat16)
    low = (value - high.astype(jnp.float32)).astype(jnp.bfloat16)
    return high, low


def put(n_size, mode, rows, xr, xi, yr, yi, x_hi, x_lo, y_all):
    start, size = rows
    at = pl.ds(mode * n_size + start, size)
    cols = pl.ds(mode * n_size, n_size)
    for part, value in enumerate((xr, xi)):
        high, low = split(value)
        lanes = pl.ds(part * n_size, n_size)
        x_hi[at, lanes] = high
        x_lo[at, lanes] = low
    for part, value in enumerate((yr, yi)):
        high, low = split(value)
        y_all[pl.ds(part * n_size + start, size), cols] = high
        y_all[pl.ds((2 + part) * n_size + start, size), cols] = low


def build_modes(n, offset, source, up, down, occ, coef, x_hi, x_lo, y_all):
    modes = up.shape[1]
    entries, n_size = source.shape[0], source.shape[2]
    chunk = 32
    for k in range(modes):
        iu = up[n, k] - offset
        iw = down[n, k] - offset
        has_u = jnp.logical_and(iu >= 0, iu < entries)
        has_w = jnp.logical_and(iw >= 0, iw < entries)
        mu = jnp.where(has_u, 1.0, 0.0).astype(jnp.float32)
        mw = jnp.where(has_w, occ[n, k], 0).astype(jnp.float32)
        iu = jnp.clip(iu, 0, entries - 1)
        iw = jnp.clip(iw, 0, entries - 1)
        a = mw * coef[0, k]
        b = mw * coef[1, k]
        for start in range(0, n_size, chunk):
            rows = pl.ds(start, chunk)
            ur, ui = source[iu, 0, rows, :], source[iu, 1, rows, :]
            wr, wi = source[iw, 0, rows, :], source[iw, 1, rows, :]
            p = ur * mu + a * wr
            q = b * wi
            r = ui * mu + a * wi
            s = b * wr
            put(n_size, k, (start, chunk), p - q, r + s, p + q, r - s, x_hi, x_lo, y_all)


def products(n_size, x_hi, x_lo, y_all, q_left, q_right):
    dot = functools.partial(jnp.dot, preferred_element_type=jnp.float32)
    both = dot(q_left[...], x_hi[...])
    left = both[:n_size] + both[n_size:] + dot(q_left[:n_size, :], x_lo[...])
    right = dot(y_all[...], q_right[...])
    two = 2 * n_size
    right = right[:two, :n_size] + right[:two, n_size:] + right[two:, :n_size]
    return left[:, :n_size] - right[:n_size], left[:, n_size:] - right[n_size:]


def local_kernel(up, down, occ, coef, rate, state, q_left, q_right, out, x_hi, x_lo, y_all):
    rows, modes = up.shape
    n_size = state.shape[2]

    @pl.loop(0, rows)
    def _(n):
        build_modes(n, 0, state, up, down, occ, coef, x_hi, x_lo, y_all)
        for start in range(0, n_size, 32):
            at = pl.ds(start, 32)
            re, im = state[n, 0, at, :], state[n, 1, at, :]
            put(n_size, modes, (start, 32), re, im, re, im, x_hi, x_lo, y_all)
            put(n_size, modes + 1, (start, 32), -im, re, -im, re, x_hi, x_lo, y_all)
        re, im = products(n_size, x_hi, x_lo, y_all, q_left, q_right)
        damping = jnp.float32(0)
        for k in range(modes):
            damping += occ[n, k].astype(jnp.float32) * rate[k]
        out[n, 0] = im - damping * state[n, 0]
        out[n, 1] = -re - damping * state[n, 1]


def remote_kernel(up, down, occ, coef, arrived, partial, q_left, q_right, out, squares, x_hi, x_lo, y_all):
    rows = up.shape[0]
    n_size = arrived.shape[2]
    squares[...] = jnp.zeros_like(squares)

    @pl.loop(0, rows)
    def _(n):
        build_modes(n, rows, arrived, up, down, occ, coef, x_hi, x_lo, y_all)
        re, im = products(n_size, x_hi, x_lo, y_all, q_left, q_right)
        re, im = partial[n, 0] + im, partial[n, 1] - re
        out[n, 0] = re
        out[n, 1] = im
        total = re * re + im * im
        squares[...] += jnp.sum(total.reshape(n_size // 8, 8, n_size), axis=0)


def pick_kernel(chosen, state, out, held, sem, load_sem):
    peers = chosen.shape[0]
    rows = state.shape[0]
    load = pltpu.make_async_copy(state, held.at[pl.ds(0, rows)], load_sem)
    load.start()
    held[rows] = jnp.zeros_like(held[rows])
    load.wait()
    copies = []
    for p in range(peers):
        at = chosen[p]
        at = jnp.where(at < 0, rows, jnp.minimum(at, rows - 1))
        copy = pltpu.make_async_copy(held.at[at], out.at[p], sem.at[p])
        copy.start()
        copies.append(copy)
    for copy in copies:
        copy.wait()


def sum_kernel(gx, gy, squares, out, gathered, send_sem, recv_sem):
    x, y = lax.axis_index("gx"), lax.axis_index("gy")
    me = x * gy + y
    count = gx * gy
    barrier = pltpu.get_barrier_semaphore()

    @pl.loop(1, count)
    def _(step):
        other = lax.rem(me + step, count)
        pl.semaphore_signal(barrier, inc=1, device_id=(other // gy, lax.rem(other, gy)), device_id_type=MESH)

    pl.semaphore_wait(barrier, count - 1)

    def copy_to(step):
        other = lax.rem(me + step, count)
        return pltpu.make_async_remote_copy(
            src_ref=squares,
            dst_ref=gathered.at[step],
            send_sem=send_sem.at[step],
            recv_sem=recv_sem.at[step],
            device_id=(other // gy, lax.rem(other, gy)),
            device_id_type=MESH,
        )

    @pl.loop(1, count)
    def _(step):
        copy_to(step).start()

    gathered[0] = squares[...]

    @pl.loop(1, count)
    def _(step):
        copy_to(step).wait()

    out[...] = jnp.sum(jnp.sum(gathered[...], axis=0), axis=(0, 1), keepdims=True) + jnp.zeros(out.shape, out.dtype)


def smem():
    return pl.BlockSpec(memory_space=pltpu.SMEM)


def vmem():
    return pl.BlockSpec(memory_space=pltpu.VMEM)


def operand_scratch(modes, n_size):
    depth = modes * n_size
    return [
        pltpu.VMEM((depth, 2 * n_size), jnp.bfloat16),
        pltpu.VMEM((depth, 2 * n_size), jnp.bfloat16),
        pltpu.VMEM((4 * n_size, depth), jnp.bfloat16),
    ]


def matrices_of(stack):
    n_size = stack.shape[1]
    high = lax.reduce_precision(stack, 8, 7)
    low = (stack - high).astype(jnp.bfloat16)
    high = high.astype(jnp.bfloat16)
    left = jnp.stack([high, low]).transpose(0, 2, 1, 3).reshape(2 * n_size, -1)
    right = jnp.stack([high, low], axis=2).reshape(-1, 2 * n_size)
    return left, right


def make_body(gx, gy):
    count = gx * gy

    def body(state, hamiltonian, couplings, bath_coef, bath_rate, occupation, send_list, up_index, down_index, step):
        rows, _, n_size, _ = state.shape
        modes = couplings.shape[0]
        chosen = send_list.reshape(-1)
        slots = chosen.shape[0]
        outgoing = pl.pallas_call(
            pick_kernel,
            out_shape=jax.ShapeDtypeStruct((slots,) + state.shape[1:], state.dtype),
            in_specs=[smem(), pl.BlockSpec(memory_space=pl.ANY)],
            out_specs=pl.BlockSpec(memory_space=pl.ANY),
            scratch_shapes=[
                pltpu.VMEM((rows + 1,) + state.shape[1:], state.dtype),
                pltpu.SemaphoreType.DMA((slots,)),
                pltpu.SemaphoreType.DMA,
            ],
            name="pick",
        )(chosen, state)
        arrived = lax.all_to_all(outgoing, AXES, split_axis=0, concat_axis=0, tiled=True)
        left, right = matrices_of(jnp.concatenate([couplings, hamiltonian], axis=0))
        pair = 2 * rows * n_size * n_size * n_size * 2
        partial = pl.pallas_call(
            local_kernel,
            out_shape=jax.ShapeDtypeStruct(state.shape, state.dtype),
            in_specs=[smem()] * 5 + [vmem()] * 3,
            out_specs=vmem(),
            scratch_shapes=operand_scratch(modes + 2, n_size),
            cost_estimate=pl.CostEstimate(flops=pair * (modes + 2) * 8, bytes_accessed=1 << 25, transcendentals=0),
            name="local",
        )(up_index, down_index, occupation, bath_coef, bath_rate, state, left, right)
        depth = modes * n_size
        derivative, squares = pl.pallas_call(
            remote_kernel,
            out_shape=(
                jax.ShapeDtypeStruct(state.shape, state.dtype),
                jax.ShapeDtypeStruct((8, n_size), state.dtype),
            ),
            in_specs=[smem()] * 4 + [vmem()] * 4,
            out_specs=(vmem(), vmem()),
            scratch_shapes=operand_scratch(modes, n_size),
            name="remote",
        )(up_index, down_index, occupation, bath_coef, arrived, partial, left[:, :depth], right[:depth])
        total = pl.pallas_call(
            functools.partial(sum_kernel, gx, gy),
            out_shape=jax.ShapeDtypeStruct((8, n_size), state.dtype),
            in_specs=[vmem()],
            out_specs=vmem(),
            scratch_shapes=[
                pltpu.VMEM((count, 8, n_size), state.dtype),
                pltpu.SemaphoreType.DMA((count,)),
                pltpu.SemaphoreType.DMA((count,)),
            ],
            compiler_params=pltpu.CompilerParams(collective_id=0, has_side_effects=True),
            name="total",
        )(squares)
        size = rows * count * 2 * n_size * n_size
        rms = jnp.sqrt(total[0, 0] / size + 1e-06)
        advanced = state + step[0] / rms * derivative
        return derivative, advanced

    return body


def solution(mesh):
    placed = (
        P(AXES, None, None, None),
        P(),
        P(),
        P(),
        P(),
        P(AXES, None),
        P(AXES, None, None),
        P(AXES, None),
        P(AXES, None),
        P(),
    )
    return jax.shard_map(
        make_body(mesh.shape["gx"], mesh.shape["gy"]),
        mesh=mesh,
        in_specs=placed,
        out_specs=(P(AXES, None, None, None), P(AXES, None, None, None)),
        check_vma=False,
    )
```

```python
import functools

import jax
import jax.numpy as jnp
from jax import lax
from jax.experimental import pallas as pl
from jax.experimental.pallas import tpu as pltpu
from jax.sharding import PartitionSpec as P

AXES = ("gx", "gy")
MESH = pl.DeviceIdType.MESH


def split(value):
    high = value.astype(jnp.bfloat16)
    low = (value - high.astype(jnp.float32)).astype(jnp.bfloat16)
    return high, low


def put(n_size, mode, rows, xr, xi, yr, yi, x_hi, x_lo, y_all):
    start, size = rows
    at = pl.ds(mode * n_size + start, size)
    cols = pl.ds(mode * n_size, n_size)
    for part, value in enumerate((xr, xi)):
        high, low = split(value)
        lanes = pl.ds(part * n_size, n_size)
        x_hi[at, lanes] = high
        x_lo[at, lanes] = low
    for part, value in enumerate((yr, yi)):
        high, low = split(value)
        y_all[pl.ds(part * n_size + start, size), cols] = high
        y_all[pl.ds((2 + part) * n_size + start, size), cols] = low


def build_modes(n, offset, source, up, down, occ, coef, x_hi, x_lo, y_all):
    modes = up.shape[1]
    entries, _, size, n_size = source[0].shape
    chunk = min(32, size)
    for k in range(modes):
        iu = up[n, k] - offset
        iw = down[n, k] - offset
        has_u = jnp.logical_and(iu >= 0, iu < entries)
        has_w = jnp.logical_and(iw >= 0, iw < entries)
        mu = jnp.where(has_u, 1.0, 0.0).astype(jnp.float32)
        mw = jnp.where(has_w, occ[n, k], 0).astype(jnp.float32)
        iu = jnp.clip(iu, 0, entries - 1)
        iw = jnp.clip(iw, 0, entries - 1)
        a = mw * coef[0, k]
        b = mw * coef[1, k]
        for start in range(0, n_size, chunk):
            part, rows = source[start // size], pl.ds(start % size, chunk)
            ur, ui = part[iu, 0, rows, :], part[iu, 1, rows, :]
            wr, wi = part[iw, 0, rows, :], part[iw, 1, rows, :]
            p = ur * mu + a * wr
            q = b * wi
            r = ui * mu + a * wi
            s = b * wr
            put(n_size, k, (start, chunk), p - q, r + s, p + q, r - s, x_hi, x_lo, y_all)


def products(n_size, x_hi, x_lo, y_all, q_left, q_right):
    dot = functools.partial(jnp.dot, preferred_element_type=jnp.float32)
    both = dot(q_left[...], x_hi[...])
    left = both[:n_size] + both[n_size:] + dot(q_left[:n_size, :], x_lo[...])
    right = dot(y_all[...], q_right[...])
    two = 2 * n_size
    right = right[:two, :n_size] + right[:two, n_size:] + right[two:, :n_size]
    return left[:, :n_size] - right[:n_size], left[:, n_size:] - right[n_size:]


def fill_matrices(mode, matrix, q_left, q_right):
    n_size = matrix.shape[0]
    high, low = split(matrix)
    at = pl.ds(mode * n_size, n_size)
    q_left[pl.ds(0, n_size), at] = high
    q_left[pl.ds(n_size, n_size), at] = low
    q_right[at, pl.ds(0, n_size)] = high
    q_right[at, pl.ds(n_size, n_size)] = low


def kernel(
    gx, gy, length, halves,
    up, down, occ, coef, rate, step, lists, state, couplings, hamiltonian,
    derivative, advanced,
    below, above, stage, arrived, list_v, list_s, x_hi, x_lo, y_all, q_left, q_right, squares, gathered,
    load_sem, up_sem, down_sem, below_sem, above_sem, list_send, list_recv, list_load, plane_send, plane_recv, sum_send, sum_recv,
):
    rows, modes = up.shape
    n_size = state.shape[2]
    count = gx * gy
    side = gy // length
    columns = gx * side
    slots = arrived.shape[0] // count
    x, y = lax.axis_index("gx"), lax.axis_index("gy")
    me = x * gy + y
    z, yy = y // side, lax.rem(y, side)
    column = x * side + yy
    size = n_size // halves

    def place(at, level):
        return at // side, level * side + lax.rem(at, side)

    def strip(half):
        return pl.ds(half * size, size)

    barrier = pltpu.get_barrier_semaphore()

    def load(half):
        return pltpu.make_async_copy(state.at[:, :, strip(half)], below[0][half], load_sem.at[half])

    for half in range(halves):
        load(half).start()

    @pl.loop(1, count)
    def _(hop):
        other = lax.rem(me + hop, count)
        pl.semaphore_signal(barrier, inc=1, device_id=(other // gy, lax.rem(other, gy)), device_id_type=MESH)

    pl.semaphore_wait(barrier, count - 1)

    def relay(hop, half, way):
        held = below if way > 0 else above
        return pltpu.make_async_remote_copy(
            src_ref=(held if hop else below)[hop][half],
            dst_ref=held[hop + 1][half],
            send_sem=(up_sem if way > 0 else down_sem).at[hop, half],
            recv_sem=(below_sem if way > 0 else above_sem).at[hop + 1, half],
            device_id=place(column, z + way),
            device_id_type=MESH,
        )

    def hand(level, hop, half, slot):
        source = place(column, level)
        return pltpu.make_async_remote_copy(
            src_ref=stage.at[level, hop, slot, :, strip(half)],
            dst_ref=arrived.at[(source[0] * gy + source[1]) * slots + slot, :, strip(half)],
            send_sem=plane_send.at[level, hop, slot, half],
            recv_sem=plane_recv.at[level, hop, slot, half],
            device_id=place(lax.rem(column + hop, columns), z),
            device_id_type=MESH,
        )

    def send_lists(hop):
        return pltpu.make_async_remote_copy(
            src_ref=lists,
            dst_ref=list_v.at[z],
            send_sem=list_send.at[hop],
            recv_sem=list_recv.at[hop],
            device_id=place(column, lax.rem(z + hop, length)),
            device_id_type=MESH,
        )

    for hop in range(1, length):
        send_lists(hop).start()
    for half in range(halves):
        load(half).wait()

        @pl.when(z + 1 < length)
        def _():
            relay(0, half, 1).start()

        @pl.when(z > 0)
        def _():
            relay(0, half, -1).start()

    own = pltpu.make_async_copy(lists, list_s.at[z], list_load.at[0])
    own.start()
    own.wait()

    def chosen(held, level, at, slot):
        target = place(at, z)
        entry = (target[0] * gy + target[1]) * slots + slot
        pick = list_s[level, entry // 128, lax.rem(entry, 128)]
        keep = jnp.where(pick < 0, 0.0, 1.0).astype(jnp.float32)
        pick = jnp.clip(pick, 0, rows - 1)
        return held[pick] * keep

    def distribute(held, level, half):
        source = place(column, level)
        first = (source[0] * gy + source[1]) * slots
        for slot in range(slots):

            @pl.loop(1, columns)
            def _(hop):
                stage[level, hop, slot, :, strip(half), :] = chosen(held, level, lax.rem(column + hop, columns), slot)
                hand(level, hop, half, slot).start()

            arrived[first + slot, :, strip(half), :] = chosen(held, level, column, slot)

    for half in range(halves):
        distribute(below[0][half], z, half)

    def arrive(hop, half):
        low, high = z - hop, z + hop

        @pl.when(low >= 0)
        def _():
            relay(hop - 1, half, 1).wait_recv()
            if hop + 1 < length:

                @pl.when(z + 1 < length)
                def _():
                    relay(hop, half, 1).start()

        @pl.when(high < length)
        def _():
            relay(hop - 1, half, -1).wait_recv()
            if hop + 1 < length:

                @pl.when(z > 0)
                def _():
                    relay(hop, half, -1).start()

        @pl.when(low >= 0)
        def _():
            distribute(below[hop][half], low, half)

        @pl.when(high < length)
        def _():
            distribute(above[hop][half], high, half)

    for k in range(modes):
        fill_matrices(k, couplings[k], q_left, q_right)
    for k in range(2):
        fill_matrices(modes + k, hamiltonian[k], q_left, q_right)
    here = below[0]

    def local_part(n):
        build_modes(n, 0, here, up, down, occ, coef, x_hi, x_lo, y_all)
        chunk = min(32, size)
        for start in range(0, n_size, chunk):
            part, at = here[start // size], pl.ds(start % size, chunk)
            re, im = part[n, 0, at, :], part[n, 1, at, :]
            put(n_size, modes, (start, chunk), re, im, re, im, x_hi, x_lo, y_all)
            put(n_size, modes + 1, (start, chunk), -im, re, -im, re, x_hi, x_lo, y_all)
        re, im = products(n_size, x_hi, x_lo, y_all, q_left, q_right)
        damping = jnp.float32(0)
        for k in range(modes):
            damping += occ[n, k].astype(jnp.float32) * rate[k]
        for half in range(halves):
            at = slice(half * size, (half + 1) * size)
            derivative[n, 0, strip(half)] = im[at] - damping * here[half][n, 0]
            derivative[n, 1, strip(half)] = -re[at] - damping * here[half][n, 1]

    for hop in range(1, length):
        send_lists(hop).wait()
    for hop in range(1, length):
        level = lax.rem(z + hop, length)
        copy = pltpu.make_async_copy(list_v.at[level], list_s.at[level], list_load.at[hop])
        copy.start()
        copy.wait()

    share = rows // halves

    for half in range(halves):

        @pl.loop(0, share)
        def _(n):
            local_part(half * share + n)

        arrive(1, half)

    for hop in range(2, length):
        for half in range(halves):
            arrive(hop, half)

    for level in range(length):

        @pl.loop(1, columns)
        def _(hop):
            for slot in range(slots):
                for half in range(halves):
                    hand(level, hop, half, slot).wait_recv()

    squares[...] = jnp.zeros_like(squares)
    depth = modes * n_size

    @pl.loop(0, rows)
    def _(n):
        build_modes(n, rows, [arrived], up, down, occ, coef, x_hi, x_lo, y_all)
        ops = (x_hi.at[:depth], x_lo.at[:depth], y_all.at[:, :depth], q_left.at[:, :depth], q_right.at[:depth])
        re, im = products(n_size, *ops)
        re, im = derivative[n, 0] + im, derivative[n, 1] - re
        derivative[n, 0] = re
        derivative[n, 1] = im
        total = re * re + im * im
        squares[...] += jnp.sum(total.reshape(n_size // 8, 8, n_size), axis=0)

    def copy_to(hop):
        other = lax.rem(me + hop, count)
        return pltpu.make_async_remote_copy(
            src_ref=squares,
            dst_ref=gathered.at[hop],
            send_sem=sum_send.at[hop],
            recv_sem=sum_recv.at[hop],
            device_id=(other // gy, lax.rem(other, gy)),
            device_id_type=MESH,
        )

    @pl.loop(1, count)
    def _(hop):
        copy_to(hop).start()

    gathered[0] = squares[...]
    for level in range(length):

        @pl.loop(1, columns)
        def _(hop):
            for slot in range(slots):
                for half in range(halves):
                    hand(level, hop, half, slot).wait_send()

    for hop in range(length - 1):
        for half in range(halves):

            @pl.when(jnp.logical_and(z >= hop, z + 1 < length))
            def _():
                relay(hop, half, 1).wait_send()

            @pl.when(jnp.logical_and(z + hop < length, z > 0))
            def _():
                relay(hop, half, -1).wait_send()

    @pl.loop(1, count)
    def _(hop):
        copy_to(hop).wait()

    total = jnp.sum(jnp.sum(gathered[...], axis=0), axis=(0, 1), keepdims=True)
    scale = step[0] / jnp.sqrt(total / (rows * count * 2 * n_size * n_size) + 1e-06)

    @pl.loop(0, rows)
    def _(n):
        for part in range(2):
            for half in range(halves):
                value = here[half][n, part] + scale * derivative[n, part, strip(half)]
                advanced[n, part, strip(half)] = value


def smem():
    return pl.BlockSpec(memory_space=pltpu.SMEM)


def vmem():
    return pl.BlockSpec(memory_space=pltpu.VMEM)


def line_length(gx, gy):
    side = max(gx // 2, 1)
    return gy // side if gy % side == 0 else gy


def make_body(gx, gy):
    count = gx * gy
    length = line_length(gx, gy)
    columns = count // length

    def body(state, hamiltonian, couplings, bath_coef, bath_rate, occupation, send_list, up_index, down_index, step):
        rows, parts, n_size, _ = state.shape
        modes = couplings.shape[0]
        slots = send_list.shape[2]
        halves = 2 if rows % 2 == 0 and n_size % 16 == 0 else 1
        chosen = send_list.reshape(-1)
        lanes = 128
        deep = -(-chosen.shape[0] // (8 * lanes)) * 8
        lists = jnp.pad(chosen, (0, deep * lanes - chosen.shape[0])).reshape(deep, lanes)
        depth = (modes + 2) * n_size
        tile = state.shape[1:]
        piece = pltpu.VMEM((rows, parts, n_size // halves, n_size), state.dtype)
        strips = tuple((piece,) * halves for _ in range(length))
        f32, bf16, i32 = jnp.float32, jnp.bfloat16, jnp.int32
        dma = pltpu.SemaphoreType.DMA
        return pl.pallas_call(
            functools.partial(kernel, gx, gy, length, halves),
            out_shape=(jax.ShapeDtypeStruct(state.shape, f32), jax.ShapeDtypeStruct(state.shape, f32)),
            in_specs=[smem()] * 6 + [vmem(), pl.BlockSpec(memory_space=pl.ANY), vmem(), vmem()],
            out_specs=(vmem(), vmem()),
            scratch_shapes=[
                strips,
                ((pltpu.VMEM((1, 1, 8, n_size), f32),) * halves,) + strips[1:],
                pltpu.VMEM((length, columns, slots) + tile, f32),
                pltpu.VMEM((count * slots,) + tile, f32),
                pltpu.VMEM((length, deep, lanes), i32),
                pltpu.SMEM((length, deep, lanes), i32),
                pltpu.VMEM((depth, 2 * n_size), bf16),
                pltpu.VMEM((depth, 2 * n_size), bf16),
                pltpu.VMEM((4 * n_size, depth), bf16),
                pltpu.VMEM((2 * n_size, depth), bf16),
                pltpu.VMEM((depth, 2 * n_size), bf16),
                pltpu.VMEM((8, n_size), f32),
                pltpu.VMEM((count, 8, n_size), f32),
                dma((halves,)),
                dma((length, halves)),
                dma((length, halves)),
                dma((length, halves)),
                dma((length, halves)),
                dma((length,)),
                dma((length,)),
                dma((length,)),
                dma((length, columns, slots, halves)),
                dma((length, columns, slots, halves)),
                dma((count,)),
                dma((count,)),
            ],
            compiler_params=pltpu.CompilerParams(collective_id=0, has_side_effects=True, vmem_limit_bytes=60 << 20),
            name="step",
        )(up_index, down_index, occupation, bath_coef, bath_rate, step, lists, state, couplings, hamiltonian)

    return body


def solution(mesh):
    placed = (
        P(AXES, None, None, None),
        P(),
        P(),
        P(),
        P(),
        P(AXES, None),
        P(AXES, None, None),
        P(AXES, None),
        P(AXES, None),
        P(),
    )
    return jax.shard_map(
        make_body(mesh.shape["gx"], mesh.shape["gy"]),
        mesh=mesh,
        in_specs=placed,
        out_specs=(P(AXES, None, None, None), P(AXES, None, None, None)),
        check_vma=False,
    )
```

```python
import functools

import jax
import jax.numpy as jnp
from jax import lax
from jax.experimental import pallas as pl
from jax.experimental.pallas import tpu as pltpu
from jax.sharding import PartitionSpec as P

AXES = ("gx", "gy")
MESH = pl.DeviceIdType.MESH


def split(value):
    high = value.astype(jnp.bfloat16)
    low = (value - high.astype(jnp.float32)).astype(jnp.bfloat16)
    return high, low


def put(n_size, mode, rows, xr, xi, yr, yi, x_hi, x_lo, y_all):
    start, size = rows
    at = pl.ds(mode * n_size + start, size)
    cols = pl.ds(mode * n_size, n_size)
    for part, value in enumerate((xr, xi)):
        high, low = split(value)
        lanes = pl.ds(part * n_size, n_size)
        x_hi[at, lanes] = high
        x_lo[at, lanes] = low
    for part, value in enumerate((yr, yi)):
        high, low = split(value)
        y_all[pl.ds(part * n_size + start, size), cols] = high
        y_all[pl.ds((2 + part) * n_size + start, size), cols] = low


def build_modes(n, offset, source, up, down, occ, coef, x_hi, x_lo, y_all):
    modes = up.shape[1]
    entries, _, size, n_size = source[0].shape
    chunk = min(32, size)
    for k in range(modes):
        iu = up[n, k] - offset
        iw = down[n, k] - offset
        has_u = jnp.logical_and(iu >= 0, iu < entries)
        has_w = jnp.logical_and(iw >= 0, iw < entries)
        mu = jnp.where(has_u, 1.0, 0.0).astype(jnp.float32)
        mw = jnp.where(has_w, occ[n, k], 0).astype(jnp.float32)
        iu = jnp.clip(iu, 0, entries - 1)
        iw = jnp.clip(iw, 0, entries - 1)
        a = mw * coef[0, k]
        b = mw * coef[1, k]
        for start in range(0, n_size, chunk):
            part, rows = source[start // size], pl.ds(start % size, chunk)
            ur, ui = part[iu, 0, rows, :], part[iu, 1, rows, :]
            wr, wi = part[iw, 0, rows, :], part[iw, 1, rows, :]
            p = ur * mu + a * wr
            q = b * wi
            r = ui * mu + a * wi
            s = b * wr
            put(n_size, k, (start, chunk), p - q, r + s, p + q, r - s, x_hi, x_lo, y_all)


def products(n_size, x_hi, x_lo, y_all, q_left, q_right):
    dot = functools.partial(jnp.dot, preferred_element_type=jnp.float32)
    both = dot(q_left[...], x_hi[...])
    left = both[:n_size] + both[n_size:] + dot(q_left[:n_size, :], x_lo[...])
    right = dot(y_all[...], q_right[...])
    two = 2 * n_size
    right = right[:two, :n_size] + right[:two, n_size:] + right[two:, :n_size]
    return left[:, :n_size] - right[:n_size], left[:, n_size:] - right[n_size:]


def fill_matrices(mode, matrix, q_left, q_right):
    n_size = matrix.shape[0]
    high, low = split(matrix)
    at = pl.ds(mode * n_size, n_size)
    q_left[pl.ds(0, n_size), at] = high
    q_left[pl.ds(n_size, n_size), at] = low
    q_right[at, pl.ds(0, n_size)] = high
    q_right[at, pl.ds(n_size, n_size)] = low


def kernel(
    gx, gy, length, halves,
    up, down, occ, coef, rate, step, lists, state, couplings, hamiltonian,
    derivative, advanced,
    below, above, stage, arrived, list_v, list_s, x_hi, x_lo, y_all, x_hi_2, x_lo_2, y_all_2, q_left, q_right, squares, gathered,
    load_sem, up_sem, down_sem, below_sem, above_sem, list_send, list_recv, list_load, plane_send, plane_recv, sum_send, sum_recv,
):
    rows, modes = up.shape
    n_size = state.shape[2]
    count = gx * gy
    side = gy // length
    columns = gx * side
    slots = arrived.shape[0] // count
    x, y = lax.axis_index("gx"), lax.axis_index("gy")
    me = x * gy + y
    z, yy = y // side, lax.rem(y, side)
    column = x * side + yy
    size = n_size // halves

    def place(at, level):
        return at // side, level * side + lax.rem(at, side)

    def strip(half):
        return pl.ds(half * size, size)

    barrier = pltpu.get_barrier_semaphore()

    def load(half):
        return pltpu.make_async_copy(state.at[:, :, strip(half)], below[0][half], load_sem.at[half])

    for half in range(halves):
        load(half).start()

    @pl.loop(1, count)
    def _(hop):
        other = lax.rem(me + hop, count)
        pl.semaphore_signal(barrier, inc=1, device_id=(other // gy, lax.rem(other, gy)), device_id_type=MESH)

    pl.semaphore_wait(barrier, count - 1)

    def relay(hop, half, way):
        held = below if way > 0 else above
        return pltpu.make_async_remote_copy(
            src_ref=(held if hop else below)[hop][half],
            dst_ref=held[hop + 1][half],
            send_sem=(up_sem if way > 0 else down_sem).at[hop, half],
            recv_sem=(below_sem if way > 0 else above_sem).at[hop + 1, half],
            device_id=place(column, z + way),
            device_id_type=MESH,
        )

    def hand(level, hop, half, slot):
        source = place(column, level)
        return pltpu.make_async_remote_copy(
            src_ref=stage.at[level, hop, slot, :, strip(half)],
            dst_ref=arrived.at[(source[0] * gy + source[1]) * slots + slot, :, strip(half)],
            send_sem=plane_send.at[level, hop, slot, half],
            recv_sem=plane_recv.at[level, hop, slot, half],
            device_id=place(lax.rem(column + hop, columns), z),
            device_id_type=MESH,
        )

    def send_lists(hop):
        return pltpu.make_async_remote_copy(
            src_ref=lists,
            dst_ref=list_v.at[z],
            send_sem=list_send.at[hop],
            recv_sem=list_recv.at[hop],
            device_id=place(column, lax.rem(z + hop, length)),
            device_id_type=MESH,
        )

    for hop in range(1, length):
        send_lists(hop).start()
    for half in range(halves):
        load(half).wait()

        @pl.when(z + 1 < length)
        def _():
            relay(0, half, 1).start()

        @pl.when(z > 0)
        def _():
            relay(0, half, -1).start()

    own = pltpu.make_async_copy(lists, list_s.at[z], list_load.at[0])
    own.start()
    own.wait()

    def chosen(held, level, at, slot):
        target = place(at, z)
        entry = (target[0] * gy + target[1]) * slots + slot
        pick = list_s[level, entry // 128, lax.rem(entry, 128)]
        keep = jnp.where(pick < 0, 0.0, 1.0).astype(jnp.float32)
        pick = jnp.clip(pick, 0, rows - 1)
        return held[pick] * keep

    def distribute(held, level, half):
        source = place(column, level)
        first = (source[0] * gy + source[1]) * slots
        for slot in range(slots):

            @pl.loop(1, columns)
            def _(hop):
                stage[level, hop, slot, :, strip(half), :] = chosen(held, level, lax.rem(column + hop, columns), slot)
                hand(level, hop, half, slot).start()

            arrived[first + slot, :, strip(half), :] = chosen(held, level, column, slot)

    for half in range(halves):
        distribute(below[0][half], z, half)

    def arrive(hop, half):
        low, high = z - hop, z + hop

        @pl.when(low >= 0)
        def _():
            relay(hop - 1, half, 1).wait_recv()
            if hop + 1 < length:

                @pl.when(z + 1 < length)
                def _():
                    relay(hop, half, 1).start()

        @pl.when(high < length)
        def _():
            relay(hop - 1, half, -1).wait_recv()
            if hop + 1 < length:

                @pl.when(z > 0)
                def _():
                    relay(hop, half, -1).start()

        @pl.when(low >= 0)
        def _():
            distribute(below[hop][half], low, half)

        @pl.when(high < length)
        def _():
            distribute(above[hop][half], high, half)

    for k in range(modes):
        fill_matrices(k, couplings[k], q_left, q_right)
    for k in range(2):
        fill_matrices(modes + k, hamiltonian[k], q_left, q_right)
    here = below[0]

    def local_part(n):
        build_modes(n, 0, here, up, down, occ, coef, x_hi, x_lo, y_all)
        chunk = min(32, size)
        for start in range(0, n_size, chunk):
            part, at = here[start // size], pl.ds(start % size, chunk)
            re, im = part[n, 0, at, :], part[n, 1, at, :]
            put(n_size, modes, (start, chunk), re, im, re, im, x_hi, x_lo, y_all)
            put(n_size, modes + 1, (start, chunk), -im, re, -im, re, x_hi, x_lo, y_all)
        re, im = products(n_size, x_hi, x_lo, y_all, q_left, q_right)
        damping = jnp.float32(0)
        for k in range(modes):
            damping += occ[n, k].astype(jnp.float32) * rate[k]
        for half in range(halves):
            at = slice(half * size, (half + 1) * size)
            derivative[n, 0, strip(half)] = im[at] - damping * here[half][n, 0]
            derivative[n, 1, strip(half)] = -re[at] - damping * here[half][n, 1]

    for hop in range(1, length):
        send_lists(hop).wait()
    for hop in range(1, length):
        level = lax.rem(z + hop, length)
        copy = pltpu.make_async_copy(list_v.at[level], list_s.at[level], list_load.at[hop])
        copy.start()
        copy.wait()

    turns = 2 if rows % 2 == 0 and halves % 2 == 0 else 1
    share, strips = rows // turns, halves // turns
    for turn in range(turns):

        @pl.loop(0, share)
        def _(n):
            local_part(turn * share + n)

        for half in range(turn * strips, (turn + 1) * strips):
            arrive(1, half)

    for hop in range(2, length):
        for half in range(halves):
            arrive(hop, half)

    for level in range(length):

        @pl.loop(1, columns)
        def _(hop):
            for slot in range(slots):
                for half in range(halves):
                    hand(level, hop, half, slot).wait_recv()

    squares[...] = jnp.zeros_like(squares)
    depth = modes * n_size

    first = (x_hi.at[:depth], x_lo.at[:depth], y_all.at[:, :depth])
    second = (x_hi_2, x_lo_2, y_all_2)

    def build(n, operands):
        build_modes(n, rows, [arrived], up, down, occ, coef, *operands)

    def finish(n, operands):
        re, im = products(n_size, *operands, q_left.at[:, :depth], q_right.at[:depth])
        re, im = derivative[n, 0] + im, derivative[n, 1] - re
        derivative[n, 0] = re
        derivative[n, 1] = im
        total = re * re + im * im
        squares[...] += jnp.sum(total.reshape(n_size // 8, 8, n_size), axis=0)

    build(0, first)

    @pl.loop(0, rows // 2)
    def _(pair):
        n = pair * 2
        build(n + 1, second)
        finish(n, first)
        build(jnp.minimum(n + 2, rows - 1), first)
        finish(n + 1, second)

    if rows % 2:
        finish(rows - 1, first)

    def copy_to(hop):
        other = lax.rem(me + hop, count)
        return pltpu.make_async_remote_copy(
            src_ref=squares,
            dst_ref=gathered.at[hop],
            send_sem=sum_send.at[hop],
            recv_sem=sum_recv.at[hop],
            device_id=(other // gy, lax.rem(other, gy)),
            device_id_type=MESH,
        )

    @pl.loop(1, count)
    def _(hop):
        copy_to(hop).start()

    gathered[0] = squares[...]
    for level in range(length):

        @pl.loop(1, columns)
        def _(hop):
            for slot in range(slots):
                for half in range(halves):
                    hand(level, hop, half, slot).wait_send()

    for hop in range(length - 1):
        for half in range(halves):

            @pl.when(jnp.logical_and(z >= hop, z + 1 < length))
            def _():
                relay(hop, half, 1).wait_send()

            @pl.when(jnp.logical_and(z + hop < length, z > 0))
            def _():
                relay(hop, half, -1).wait_send()

    @pl.loop(1, count)
    def _(hop):
        copy_to(hop).wait()

    total = jnp.sum(jnp.sum(gathered[...], axis=0), axis=(0, 1), keepdims=True)
    scale = step[0] / jnp.sqrt(total / (rows * count * 2 * n_size * n_size) + 1e-06)

    @pl.loop(0, rows)
    def _(n):
        for part in range(2):
            for half in range(halves):
                value = here[half][n, part] + scale * derivative[n, part, strip(half)]
                advanced[n, part, strip(half)] = value


def smem():
    return pl.BlockSpec(memory_space=pltpu.SMEM)


def vmem():
    return pl.BlockSpec(memory_space=pltpu.VMEM)


def line_length(gx, gy):
    side = max(gx // 2, 1)
    return gy // side if gy % side == 0 else gy


def make_body(gx, gy):
    count = gx * gy
    length = line_length(gx, gy)
    columns = count // length

    def body(state, hamiltonian, couplings, bath_coef, bath_rate, occupation, send_list, up_index, down_index, step):
        rows, parts, n_size, _ = state.shape
        modes = couplings.shape[0]
        slots = send_list.shape[2]
        halves = 4 if n_size % 32 == 0 else 1
        chosen = send_list.reshape(-1)
        lanes = 128
        deep = -(-chosen.shape[0] // (8 * lanes)) * 8
        lists = jnp.pad(chosen, (0, deep * lanes - chosen.shape[0])).reshape(deep, lanes)
        depth = (modes + 2) * n_size
        tile = state.shape[1:]
        piece = pltpu.VMEM((rows, parts, n_size // halves, n_size), state.dtype)
        strips = tuple((piece,) * halves for _ in range(length))
        f32, bf16, i32 = jnp.float32, jnp.bfloat16, jnp.int32
        dma = pltpu.SemaphoreType.DMA
        return pl.pallas_call(
            functools.partial(kernel, gx, gy, length, halves),
            out_shape=(jax.ShapeDtypeStruct(state.shape, f32), jax.ShapeDtypeStruct(state.shape, f32)),
            in_specs=[smem()] * 6 + [vmem(), pl.BlockSpec(memory_space=pl.ANY), vmem(), vmem()],
            out_specs=(vmem(), vmem()),
            scratch_shapes=[
                strips,
                ((pltpu.VMEM((1, 1, 8, n_size), f32),) * halves,) + strips[1:],
                pltpu.VMEM((length, columns, slots) + tile, f32),
                pltpu.VMEM((count * slots,) + tile, f32),
                pltpu.VMEM((length, deep, lanes), i32),
                pltpu.SMEM((length, deep, lanes), i32),
                pltpu.VMEM((depth, 2 * n_size), bf16),
                pltpu.VMEM((depth, 2 * n_size), bf16),
                pltpu.VMEM((4 * n_size, depth), bf16),
                pltpu.VMEM((modes * n_size, 2 * n_size), bf16),
                pltpu.VMEM((modes * n_size, 2 * n_size), bf16),
                pltpu.VMEM((4 * n_size, modes * n_size), bf16),
                pltpu.VMEM((2 * n_size, depth), bf16),
                pltpu.VMEM((depth, 2 * n_size), bf16),
                pltpu.VMEM((8, n_size), f32),
                pltpu.VMEM((count, 8, n_size), f32),
                dma((halves,)),
                dma((length, halves)),
                dma((length, halves)),
                dma((length, halves)),
                dma((length, halves)),
                dma((length,)),
                dma((length,)),
                dma((length,)),
                dma((length, columns, slots, halves)),
                dma((length, columns, slots, halves)),
                dma((count,)),
                dma((count,)),
            ],
            compiler_params=pltpu.CompilerParams(collective_id=0, has_side_effects=True, vmem_limit_bytes=60 << 20),
            name="step",
        )(up_index, down_index, occupation, bath_coef, bath_rate, step, lists, state, couplings, hamiltonian)

    return body


def solution(mesh):
    placed = (
        P(AXES, None, None, None),
        P(),
        P(),
        P(),
        P(),
        P(AXES, None),
        P(AXES, None, None),
        P(AXES, None),
        P(AXES, None),
        P(),
    )
    return jax.shard_map(
        make_body(mesh.shape["gx"], mesh.shape["gy"]),
        mesh=mesh,
        in_specs=placed,
        out_specs=(P(AXES, None, None, None), P(AXES, None, None, None)),
        check_vma=False,
    )
```
